512 devices in a mesh: rows: 512 (over z, y, x, core).
Axes of the slice: x: 4, y: 8, z: 8, core: 2. Of those that a mesh axis runs over, the one named last changes fastest.
Arguments:
- adj_diag: int32 [8192, 512], P('rows'), may hold values from -2147483648 to 2147483647
- adj_right: int32 [8192, 512], P('rows'), may hold values from -2147483648 to 2147483647
- alive_diag: int32 [8192, 512], P('rows'), may hold values from -2147483648 to 2147483647
- alive_right: int32 [8192, 512], P('rows'), may hold values from -2147483648 to 2147483647
- truss_k: int32 [1], replicated, may hold values from 130 to 193
Outputs:
- support_field: float32 [262144, 1024], P('rows')
- removed_counts: int32 [3], replicated
The draws below stay inside these ranges and needn't reach their ends.
All inputs are finite; a program needn't handle non-finite values.
Results may differ from the reference program's by a relative error of at most 0.0003.
Values may be sent and summed in bfloat16 or wider, within the bound.
A program may use at most 64 MiB of HBM per device.

```python
import jax
import jax.numpy as jnp
from jax import lax

TILE = 512
ITERS = 3
NVERT = 262144


def vertex_levels(key, block):
    base_key = jax.random.fold_in(jax.random.fold_in(key, 7001), block)
    size_key, order_key, level_key = jax.random.split(base_key, 3)
    core_count = jax.random.randint(size_key, (), TILE // 4, 3 * TILE // 8 + 1, dtype=jnp.int32)
    order = jax.random.permutation(order_key, TILE)
    is_core = order < core_count
    levels = jax.random.randint(level_key, (TILE,), 2, 16, dtype=jnp.int32)
    return (jnp.where(is_core, jnp.int32(16), levels), is_core)


def pack_bits(tile_bits):
    shifts = jnp.arange(32, dtype=jnp.int32)
    sectioned = tile_bits.reshape(TILE // 32, 32, TILE)
    return jnp.sum(sectioned << shifts[None, :, None], axis=1, dtype=jnp.int32)


def draw_bits(key, salt, offset, alive_kind):
    blocks = NVERT // TILE

    def one_block(block):
        row_levels, row_core = vertex_levels(key, block)
        col_levels, col_core = vertex_levels(key, (block + offset) % blocks)
        edge_key = jax.random.fold_in(jax.random.fold_in(key, salt), block)
        if alive_kind:
            chance = jax.random.randint(edge_key, (TILE, TILE), 0, 8, dtype=jnp.int32)
            both_core = row_core[:, None] & col_core[None, :]
            tile_bits = jnp.where(both_core, jnp.int32(1), (chance < 7).astype(jnp.int32))
        else:
            chance = jax.random.randint(edge_key, (TILE, TILE), 0, 256, dtype=jnp.int32)
            tile_bits = (chance < row_levels[:, None] * col_levels[None, :]).astype(jnp.int32)
        return pack_bits(tile_bits)
    packed = lax.map(one_block, jnp.arange(blocks, dtype=jnp.int32))
    return packed.reshape(NVERT // 32, TILE)


def draw_adj_diag(key, part):
    return draw_bits(key, 101, 0, False)


def draw_adj_right(key, part):
    return draw_bits(key, 102, 1, False)


def draw_alive_diag(key, part):
    return draw_bits(key, 103, 0, True)


def draw_alive_right(key, part):
    return draw_bits(key, 104, 1, True)


def setup_inputs(seed: int = 0) -> dict:
    seeds = jax.random.split(jax.random.key(seed), 6)
    adj_diag = draw_adj_diag(jax.random.fold_in(seeds[5], 71), 0)
    adj_right = draw_adj_right(jax.random.fold_in(seeds[5], 71), 0)
    alive_diag = draw_alive_diag(jax.random.fold_in(seeds[5], 71), 0)
    alive_right = draw_alive_right(jax.random.fold_in(seeds[5], 71), 0)
    truss_k = jax.random.randint(seeds[4], (1,), TILE // 4 + 2, 3 * TILE // 8 + 2).astype(jnp.int32)
    return {"adj_diag": adj_diag, "adj_right": adj_right, "alive_diag": alive_diag, "alive_right": alive_right, "truss_k": truss_k}


def unpack_tiles(packed, blocks, tile):
    shifts = jnp.arange(32, dtype=jnp.int32)
    sectioned = packed.reshape(blocks, tile // 32, tile)
    tile_bits = (sectioned[:, :, None, :] >> shifts[None, None, :, None]) & 1
    return tile_bits.reshape(blocks, tile, tile)


def tile_support(pieces):
    within, across, prev_across, next_within = pieces
    inside = lax.dot_general(prev_across, prev_across, (((0,), (0,)), ((), ())), preferred_element_type=jnp.float32)
    inside = inside + jnp.dot(within, within, preferred_element_type=jnp.float32)
    inside = inside + lax.dot_general(across, across, (((1,), (1,)), ((), ())), preferred_element_type=jnp.float32)
    between = jnp.dot(within, across, preferred_element_type=jnp.float32)
    between = between + jnp.dot(across, next_within, preferred_element_type=jnp.float32)
    return inside, between


def reference(adj_diag, adj_right, alive_diag, alive_right, truss_k):
    blocks = NVERT // TILE
    upper_half = jnp.triu(unpack_tiles(adj_diag & alive_diag, blocks, TILE), 1)
    within = (upper_half + jnp.swapaxes(upper_half, 1, 2)).astype(jnp.bfloat16)
    across = unpack_tiles(adj_right & alive_right, blocks, TILE).astype(jnp.bfloat16)
    thresh = (truss_k[0] - 2).astype(jnp.float32)
    counts = []
    for step in range(ITERS):
        prev_across = jnp.roll(across, 1, axis=0)
        next_within = jnp.roll(within, -1, axis=0)
        inside, between = lax.map(tile_support, (within, across, prev_across, next_within))
        new_within = jnp.where(inside >= thresh, within, jnp.zeros_like(within))
        new_across = jnp.where(between >= thresh, across, jnp.zeros_like(across))
        lost_within = jnp.sum((within - new_within).astype(jnp.int32)) // 2
        lost_across = jnp.sum((across - new_across).astype(jnp.int32))
        counts.append(lost_within + lost_across)
        within, across = new_within, new_across
    support = jnp.concatenate([inside * within.astype(jnp.float32), between * across.astype(jnp.float32)], axis=2)
    return support.reshape(NVERT, 2 * TILE), jnp.stack(counts).astype(jnp.int32)
```

```python
import jax
import jax.numpy as jnp
from jax import lax
from jax.experimental import pallas as pl
from jax.experimental.pallas import tpu as pltpu
from jax.sharding import PartitionSpec as P

TILE = 512
WORDS = TILE // 32
HALF = 4
F8 = jnp.float8_e4m3fn
F32 = jnp.float32
I32 = jnp.int32
MESH = pl.DeviceIdType.MESH
CORE, XAX, YAX, ZAX = (1, 2), (2, 4), (8, 8), (64, 8)
PHASES = ((CORE,), (XAX,), (YAX,), (ZAX,))


def rows_index():
    return lax.axis_index("rows")


def signal(sem, device):
    pl.semaphore_signal(sem, inc=1, device_id=(device,), device_id_type=MESH)


def exchange_kernel(n, ad, ar, ld, lr, acr, wit, send_sem, recv_sem):
    me = rows_index()
    barrier = pltpu.get_barrier_semaphore()
    dev = {k: lax.rem(me + k + n, n) for k in (-2, -1, 1, 2)}
    for k in dev:
        signal(barrier, dev[k])
    acr[2] = ar[...] & lr[...]
    wit[1] = ad[...] & ld[...]
    pl.semaphore_wait(barrier, 4)
    plan = (
        (acr, 2, 1, 1), (wit, 1, -1, 2), (acr, 2, -1, 3), (wit, 1, 1, 0),
        (acr, 2, 2, 0), (wit, 1, -2, 3),
    )
    copies = []
    for i, (ref, src, to, dst) in enumerate(plan):
        copies.append(
            pltpu.make_async_remote_copy(
                src_ref=ref.at[src], dst_ref=ref.at[dst],
                send_sem=send_sem.at[i], recv_sem=recv_sem.at[i],
                device_id=(dev[to],), device_id_type=MESH,
            )
        )
        copies[-1].start()
    for c in copies:
        c.wait_recv()
    for c in copies:
        c.wait_send()


def peer_list(me, phase):
    offsets = [0]
    ids = [me]
    for stride, size in phase:
        pos = lax.rem(lax.div(me, stride), size)
        new = []
        for base in ids:
            for k in range(size):
                other = lax.rem(pos + k, size)
                new.append(base + (other - pos) * stride)
        ids = new
    return ids[1:]


def dot(a, b):
    return jnp.dot(a, b, preferred_element_type=F32)


def dot_tn(a, b):
    return lax.dot_general(a, b, (((0,), (0,)), ((), ())), preferred_element_type=F32)


def dot_nt(a, b):
    return lax.dot_general(a, b, (((1,), (1,)), ((), ())), preferred_element_type=F32)


def unpack(words):
    bit = lax.broadcasted_iota(I32, (32, TILE), 0)
    return (words >> bit) & 1


def peel_kernel(th_ref, acr, wit, sup, cnt_ref, A, W, U, sbuf, rbuf, send_sem, recv_sem):
    me = rows_index()
    barrier = pltpu.get_barrier_semaphore()
    peers = [peer_list(me, p) for p in PHASES]
    for group in peers:
        for d in group:
            signal(barrier, d)
    thresh = (th_ref[0] - 2).astype(F32)

    def open_across(t, _):
        for g in range(WORDS):
            A[0, t, 32 * g:32 * g + 32, :] = unpack(acr[t, g:g + 1, :]).astype(F32).astype(F8)
        return 0

    def open_within(t, _):
        for g in range(WORDS):
            r = lax.broadcasted_iota(I32, (32, TILE), 0) + 32 * g
            c = lax.broadcasted_iota(I32, (32, TILE), 1)
            U[32 * g:32 * g + 32, :] = jnp.where(c > r, unpack(wit[t, g:g + 1, :]), 0).astype(F32)
        u = U[...]
        W[0, t] = (u + u.T).astype(F8)
        return 0

    lax.fori_loop(0, HALF, open_across, 0)
    lax.fori_loop(0, HALF, open_within, 0)

    def inside(s, j):
        return (
            dot_tn(A[s, j], A[s, j]) + dot(W[s, j], W[s, j]) + dot_nt(A[s, j + 1], A[s, j + 1])
        )

    def between(s, j):
        return dot(W[s, j], A[s, j + 1]) + dot(A[s, j + 1], W[s, j + 1])

    def keep(x, old):
        return jnp.where(x >= thresh, old.astype(F32), 0.0)

    def edges(w, a):
        s = jnp.sum(w, axis=0, keepdims=True) * 0.5 + jnp.sum(a, axis=0, keepdims=True)
        return jnp.sum(s, axis=1, keepdims=True)

    def held(s):
        return edges(W[s, 1].astype(F32), A[s, 2].astype(F32))

    total = [held(0)]
    for j in range(3):
        W[1, j] = keep(inside(0, j), W[0, j]).astype(F8)
        A[1, j + 1] = keep(between(0, j), A[0, j + 1]).astype(F8)
    total.append(held(1))
    for j in range(2):
        A[0, j + 1] = keep(between(1, j), A[1, j + 1]).astype(F8)
        W[0, j + 1] = keep(inside(1, j + 1), W[1, j + 1]).astype(F8)
    total.append(held(0))
    x = inside(0, 1)
    w = keep(x, W[0, 1])
    sup[:, :TILE] = x * w
    x = between(0, 1)
    a = keep(x, A[0, 2])
    sup[:, TILE:] = x * a
    total.append(edges(w, a))

    lane = lax.broadcasted_iota(I32, (1, 128), 1)
    acc = jnp.zeros((1, 128), I32)
    for i in range(3):
        lost = (total[i] - total[i + 1]).astype(I32)
        acc = jnp.where(lane == i, lost, acc)

    pl.semaphore_wait(barrier, sum(len(g) for g in peers))
    sends = []
    for p, group in enumerate(peers):
        sbuf[p:p + 1, :] = acc
        copies = []
        for k, d in enumerate(group):
            copies.append(
                pltpu.make_async_remote_copy(
                    src_ref=sbuf.at[pl.ds(p, 1)], dst_ref=rbuf.at[p, pl.ds(k, 1)],
                    send_sem=send_sem.at[p, k], recv_sem=recv_sem.at[p, k],
                    device_id=(d,), device_id_type=MESH,
                )
            )
            copies[-1].start()
        for c in copies:
            c.wait_recv()
        for k in range(len(group)):
            acc = acc + rbuf[p, k:k + 1, :]
        sends += copies
    cnt_ref[...] = acc
    for c in sends:
        c.wait_send()


def on_device(adj_diag, adj_right, alive_diag, alive_right, truss_k):
    n = lax.axis_size("rows")
    vmem = pl.BlockSpec(memory_space=pltpu.VMEM)
    words = jax.ShapeDtypeStruct((HALF, WORDS, TILE), I32)
    acr, wit = pl.pallas_call(
        lambda *refs: exchange_kernel(n, *refs),
        out_shape=(words, words),
        in_specs=[vmem] * 4,
        out_specs=[vmem] * 2,
        scratch_shapes=[pltpu.SemaphoreType.DMA((6,)), pltpu.SemaphoreType.DMA((6,))],
        compiler_params=pltpu.CompilerParams(collective_id=0, has_side_effects=True),
        name="exchange",
    )(adj_diag, adj_right, alive_diag, alive_right)
    most = max(len_of(p) for p in PHASES)
    support, counts = pl.pallas_call(
        peel_kernel,
        out_shape=(
            jax.ShapeDtypeStruct((TILE, 2 * TILE), F32),
            jax.ShapeDtypeStruct((1, 128), I32),
        ),
        in_specs=[pl.BlockSpec(memory_space=pltpu.SMEM), vmem, vmem],
        out_specs=[vmem, vmem],
        scratch_shapes=[
            pltpu.VMEM((2, HALF, TILE, TILE), F8),
            pltpu.VMEM((2, HALF, TILE, TILE), F8),
            pltpu.VMEM((TILE, TILE), F32),
            pltpu.VMEM((len(PHASES), 128), I32),
            pltpu.VMEM((len(PHASES), most, 128), I32),
            pltpu.SemaphoreType.DMA((len(PHASES), most)),
            pltpu.SemaphoreType.DMA((len(PHASES), most)),
        ],
        compiler_params=pltpu.CompilerParams(
            collective_id=1, has_side_effects=True, vmem_limit_bytes=56 * 2**20
        ),
        name="peel",
    )(truss_k, acr, wit)
    return support, counts[0, :3]


def len_of(phase):
    size = 1
    for _, s in phase:
        size *= s
    return size - 1


def solution(mesh):
    rows = P("rows", None)
    return jax.shard_map(
        on_device, mesh=mesh, in_specs=(rows, rows, rows, rows, P(None)),
        out_specs=(rows, P(None)), check_vma=False,
    )
```

```python
import jax
import jax.numpy as jnp
from jax import lax
from jax.experimental import pallas as pl
from jax.experimental.pallas import tpu as pltpu
from jax.sharding import PartitionSpec as P

TILE = 512
WORDS = TILE // 32
HALF = 4
F8 = jnp.float8_e4m3fn
F32 = jnp.float32
I32 = jnp.int32
MESH = pl.DeviceIdType.MESH
XAX, YAX, ZAX = (2, 4), (8, 8), (64, 8)
GATHER = (YAX,)
SPREAD = (XAX, ZAX)


def chips_of(chip, axes):
    ids = [chip]
    for stride, size in axes:
        pos = lax.rem(lax.div(chip, stride), size)
        ids = [
            base + (lax.rem(pos + k, size) - pos) * stride if k else base
            for base in ids for k in range(size)
        ]
    return ids


def dot(a, b):
    return jnp.dot(a, b, preferred_element_type=F32)


def dot_tn(a, b):
    return lax.dot_general(a, b, (((0,), (0,)), ((), ())), preferred_element_type=F32)


def dot_nt(a, b):
    return lax.dot_general(a, b, (((1,), (1,)), ((), ())), preferred_element_type=F32)


def unpack(words):
    bit = lax.broadcasted_iota(I32, (32, TILE), 0)
    return (words >> bit) & 1


def peel_kernel(
    n, ad, ar, ld, lr, th_ref, sup, cnt_ref,
    raw, acr, wit, A, W, U, Pw, Qa, sbuf, rbuf,
    in_sem, x_send, x_recv, r_send, r_recv,
):
    me = lax.axis_index("rows")
    core = lax.rem(me, 2)
    chip = me - core
    mate = chip + 1 - core
    gather = chips_of(chip, GATHER)
    spread = chips_of(chip, SPREAD)
    dev = {k: lax.rem(me + k + n, n) for k in (-2, -1, 1, 2)}

    loads = [
        pltpu.make_async_copy(src, raw.at[i], in_sem.at[i])
        for i, src in enumerate((ar, lr, ad, ld))
    ]
    for c in loads:
        c.start()

    barrier = pltpu.get_barrier_semaphore()

    def signal(device):
        pl.semaphore_signal(barrier, inc=1, device_id=(device,), device_id_type=MESH)

    for k in dev:
        signal(dev[k])

    signal(mate)
    for c in gather[1:] + spread[1:]:
        signal(c + 1)

    @pl.when(core == 1)
    def _():
        for c in gather[1:] + spread[1:]:
            signal(c)

    loads[0].wait()
    loads[1].wait()
    acr[2] = raw[0] & raw[1]
    loads[2].wait()
    loads[3].wait()
    wit[1] = raw[2] & raw[3]
    even_count = 4 + len(gather) + len(spread) - 1

    @pl.when(core == 0)
    def _():
        pl.semaphore_wait(barrier, even_count)

    @pl.when(core == 1)
    def _():
        pl.semaphore_wait(barrier, even_count + len(gather) + len(spread) - 2)

    plan = (
        (acr, 2, 1, 1), (wit, 1, -1, 2), (wit, 1, 1, 0), (acr, 2, -1, 3),
        (acr, 2, 2, 0), (wit, 1, -2, 3),
    )
    moves = []
    for i, (ref, src, to, dst) in enumerate(plan):
        moves.append(
            pltpu.make_async_remote_copy(
                src_ref=ref.at[src], dst_ref=ref.at[dst],
                send_sem=x_send.at[i], recv_sem=x_recv.at[i],
                device_id=(dev[to],), device_id_type=MESH,
            )
        )
        moves[-1].start()

    thresh = (th_ref[0] - 2).astype(F32)

    def open_across(t):
        for g in range(WORDS):
            A[0, t, 32 * g:32 * g + 32, :] = unpack(acr[t, g:g + 1, :]).astype(F32).astype(F8)

    def open_within(t):
        for g in range(WORDS):
            r = lax.broadcasted_iota(I32, (32, TILE), 0) + 32 * g
            c = lax.broadcasted_iota(I32, (32, TILE), 1)
            U[32 * g:32 * g + 32, :] = jnp.where(c > r, unpack(wit[t, g:g + 1, :]), 0).astype(F32)
        u = U[...]
        W[0, t] = (u + u.T).astype(F8)

    def keep(x, old):
        return jnp.where(x >= thresh, old.astype(F32), 0.0)

    def edges(w, a):
        s = jnp.sum(w, axis=0, keepdims=True) * 0.5 + jnp.sum(a, axis=0, keepdims=True)
        return jnp.sum(s, axis=1, keepdims=True)

    def inside(s, j):
        return (
            dot_tn(A[s, j], A[s, j]) + dot(W[s, j], W[s, j]) + dot_nt(A[s, j + 1], A[s, j + 1])
        )

    def between(s, j):
        return dot(W[s, j], A[s, j + 1]) + dot(A[s, j + 1], W[s, j + 1])

    open_across(2)
    open_within(1)
    a = A[0, 2]
    w = W[0, 1]
    total = [edges(w.astype(F32), a.astype(F32))]
    Pw[...] = dot(w, w) + dot_nt(a, a)
    Qa[...] = dot(w, a)

    for c in moves[:4]:
        c.wait_recv()
    open_across(1)
    open_within(2)
    open_within(0)
    open_across(3)
    w = keep(dot_tn(A[0, 1], A[0, 1]) + Pw[...], W[0, 1])
    W[1, 1] = w.astype(F8)
    a = keep(dot(A[0, 2], W[0, 2]) + Qa[...], A[0, 2])
    A[1, 2] = a.astype(F8)
    total.append(edges(w, a))
    A[1, 1] = keep(between(0, 0), A[0, 1]).astype(F8)
    W[1, 2] = keep(inside(0, 2), W[0, 2]).astype(F8)

    for c in moves[4:]:
        c.wait_recv()
    open_across(0)
    open_within(3)
    W[1, 0] = keep(inside(0, 0), W[0, 0]).astype(F8)
    A[1, 3] = keep(between(0, 2), A[0, 3]).astype(F8)

    A[0, 1] = keep(between(1, 0), A[1, 1]).astype(F8)
    W[0, 2] = keep(inside(1, 2), W[1, 2]).astype(F8)
    w = keep(inside(1, 1), W[1, 1])
    W[0, 1] = w.astype(F8)
    a = keep(between(1, 1), A[1, 2])
    A[0, 2] = a.astype(F8)
    total.append(edges(w, a))

    x = inside(0, 1)
    sup[:, :TILE] = x
    w = keep(x, W[0, 1])
    y = between(0, 1)
    sup[:, TILE:] = y
    a = keep(y, A[0, 2])
    total.append(edges(w, a))

    lane = lax.broadcasted_iota(I32, (1, 128), 1)
    acc = jnp.zeros((1, 128), I32)
    for i in range(3):
        lost = (total[i] - total[i + 1]).astype(I32)
        acc = jnp.where(lane == i, lost, acc)
    sbuf[0:1, :] = acc
    rbuf[0, 1:2, :] = acc

    def send(stage, slot, device, k):
        return pltpu.make_async_remote_copy(
            src_ref=sbuf.at[pl.ds(stage, 1)], dst_ref=rbuf.at[stage, pl.ds(slot, 1)],
            send_sem=r_send.at[stage, k], recv_sem=r_recv.at[stage, slot],
            device_id=(device,), device_id_type=MESH,
        )

    far = range(len(gather) - 1, -1, -1)

    @pl.when(core == 0)
    def _():
        for k in far:
            send(0, 2 * k, gather[k] + 1, k).start()

    @pl.when(core == 1)
    def _():
        for k in far[:-1]:
            send(0, 2 * k + 1, gather[k] + 1, k).start()

    sup[:, :TILE] = sup[:, :TILE] * jnp.where(
        sup[:, :TILE] >= thresh, W[0, 1].astype(F32), 0.0)
    sup[:, TILE:] = sup[:, TILE:] * jnp.where(
        sup[:, TILE:] >= thresh, A[0, 2].astype(F32), 0.0)

    @pl.when(core == 1)
    def _():
        for k in range(len(gather)):
            for c in (0, 1):
                if k or not c:
                    send(0, 2 * k + c, mate, k).wait_recv()
        part = jnp.sum(rbuf[0, 0:2 * len(gather), :], axis=0, keepdims=True)
        sbuf[1:2, :] = part
        rbuf[1, 0:1, :] = part
        count = len(spread)
        for k in range(count - 1, -1, -1):
            if k:
                send(1, k, spread[k] + 1, k).start()
            send(1, k, spread[k], count + k).start()
        for k in range(1, count):
            send(1, k, mate, k).wait_recv()

    @pl.when(core == 0)
    def _():
        for k in range(len(spread)):
            send(1, k, mate, k).wait_recv()

    cnt_ref[...] = jnp.sum(rbuf[1, 0:len(spread), :], axis=0, keepdims=True)

    for c in moves:
        c.wait_send()

    @pl.when(core == 0)
    def _():
        for k in far:
            send(0, 2 * k, mate, k).wait_send()

    @pl.when(core == 1)
    def _():
        for k in far[:-1]:
            send(0, 2 * k + 1, mate, k).wait_send()
        for k in range(2 * len(spread)):
            if k:
                send(1, 0, mate, k).wait_send()


def write_kernel(sup, cnt, out, counts, sem):
    copies = [
        pltpu.make_async_copy(sup.at[pl.ds(128 * i, 128)], out.at[pl.ds(128 * i, 128)], sem.at[i])
        for i in range(4)
    ]
    for c in copies:
        c.start()
    counts[...] = cnt[0, :3]
    for c in copies:
        c.wait()


def group_size(axes):
    size = 1
    for _, s in axes:
        size *= s
    return size


def on_device(adj_diag, adj_right, alive_diag, alive_right, truss_k):
    n = lax.axis_size("rows")
    vmem = pl.BlockSpec(memory_space=pltpu.VMEM)
    smem = pl.BlockSpec(memory_space=pltpu.SMEM)
    hbm = pl.BlockSpec(memory_space=pl.ANY)
    slots = max(2 * group_size(GATHER), 2 * group_size(SPREAD))
    tiles = [
        pltpu.with_memory_space_constraint(x, pltpu.HBM)
        for x in (adj_diag, adj_right, alive_diag, alive_right)
    ]
    support, counts = pl.pallas_call(
        lambda *refs: peel_kernel(n, *refs),
        out_shape=(
            pltpu.VMEM((TILE, 2 * TILE), F32),
            pltpu.VMEM((1, 128), I32),
        ),
        in_specs=[pl.BlockSpec(memory_space=pltpu.HBM)] * 4 + [smem],
        out_specs=[vmem, vmem],
        scratch_shapes=[
            pltpu.VMEM((4, WORDS, TILE), I32),
            pltpu.VMEM((HALF, WORDS, TILE), I32),
            pltpu.VMEM((HALF, WORDS, TILE), I32),
            pltpu.VMEM((2, HALF, TILE, TILE), F8),
            pltpu.VMEM((2, HALF, TILE, TILE), F8),
            pltpu.VMEM((TILE, TILE), F32),
            pltpu.VMEM((TILE, TILE), F32),
            pltpu.VMEM((TILE, TILE), F32),
            pltpu.VMEM((2, 128), I32),
            pltpu.VMEM((2, slots, 128), I32),
            pltpu.SemaphoreType.DMA((4,)),
            pltpu.SemaphoreType.DMA((6,)),
            pltpu.SemaphoreType.DMA((6,)),
            pltpu.SemaphoreType.DMA((2, slots)),
            pltpu.SemaphoreType.DMA((2, slots)),
        ],
        compiler_params=pltpu.CompilerParams(
            collective_id=0, has_side_effects=True, vmem_limit_bytes=40 * 2**20
        ),
        name="peel",
    )(*tiles, truss_k)
    return pl.pallas_call(
        write_kernel,
        out_shape=(
            jax.ShapeDtypeStruct((TILE, 2 * TILE), F32),
            jax.ShapeDtypeStruct((3,), I32),
        ),
        in_specs=[vmem, vmem],
        out_specs=[hbm, vmem],
        scratch_shapes=[pltpu.SemaphoreType.DMA((4,))],
        compiler_params=pltpu.CompilerParams(vmem_limit_bytes=4 * 2**20),
        name="write",
    )(support, counts)


def solution(mesh):
    rows = P("rows", None)
    return jax.shard_map(
        on_device, mesh=mesh, in_specs=(rows, rows, rows, rows, P(None)),
        out_specs=(rows, P(None)), check_vma=False,
    )
```

```python
import jax
import jax.numpy as jnp
from jax import lax
from jax.experimental import pallas as pl
from jax.experimental.pallas import tpu as pltpu
from jax.sharding import PartitionSpec as P

TILE = 512
WORDS = TILE // 32
HALF = 4
F8 = jnp.float8_e4m3fn
F32 = jnp.float32
I32 = jnp.int32
MESH = pl.DeviceIdType.MESH
XAX, YAX, ZAX = (2, 4), (8, 8), (64, 8)
GATHER = (YAX,)
SPREAD = (XAX, ZAX)


def chips_of(chip, axes):
    ids = [chip]
    for stride, size in axes:
        pos = lax.rem(lax.div(chip, stride), size)
        ids = [
            base + (lax.rem(pos + k, size) - pos) * stride if k else base
            for base in ids for k in range(size)
        ]
    return ids


def dot(a, b):
    return jnp.dot(a, b, preferred_element_type=F32)


def dot_tn(a, b):
    return lax.dot_general(a, b, (((0,), (0,)), ((), ())), preferred_element_type=F32)


def dot_nt(a, b):
    return lax.dot_general(a, b, (((1,), (1,)), ((), ())), preferred_element_type=F32)


def unpack(words):
    bit = lax.broadcasted_iota(I32, (32, TILE), 0)
    return (words >> bit) & 1


def peel_kernel(
    n, ad, ar, ld, lr, th_ref, sup, cnt_ref,
    raw, acr, wit, A, W, U, Pw, Qa, sbuf, buf1, buf2, buf3,
    in_sem, x_send, x_recv, r_send, r_recv,
):
    me = lax.axis_index("rows")
    core = lax.rem(me, 2)
    chip = me - core
    mate = chip + 1 - core
    gather = chips_of(chip, GATHER)
    spread = chips_of(chip, SPREAD)
    dev = {k: lax.rem(me + k + n, n) for k in (-2, -1, 1, 2)}

    loads = [
        pltpu.make_async_copy(src, raw.at[i], in_sem.at[i])
        for i, src in enumerate((ar, lr, ad, ld))
    ]
    for c in loads:
        c.start()

    barrier = pltpu.get_barrier_semaphore()

    def signal(device):
        pl.semaphore_signal(barrier, inc=1, device_id=(device,), device_id_type=MESH)

    for k in dev:
        signal(dev[k])

    signal(mate)
    for c in gather[1:]:
        signal(c + 1)

    @pl.when(core == 1)
    def _():
        for c in gather[1:]:
            signal(c)
        for c in spread[1:]:
            signal(c + 1)

    loads[0].wait()
    loads[1].wait()
    acr[2] = raw[0] & raw[1]
    loads[2].wait()
    loads[3].wait()
    wit[1] = raw[2] & raw[3]
    even_count = 4 + len(gather)

    @pl.when(core == 0)
    def _():
        pl.semaphore_wait(barrier, even_count)

    @pl.when(core == 1)
    def _():
        pl.semaphore_wait(barrier, even_count + len(gather) + len(spread) - 2)

    plan = (
        (acr, 2, 1, 1), (wit, 1, -1, 2), (wit, 1, 1, 0), (acr, 2, -1, 3),
        (acr, 2, 2, 0), (wit, 1, -2, 3),
    )
    moves = []
    for i, (ref, src, to, dst) in enumerate(plan):
        moves.append(
            pltpu.make_async_remote_copy(
                src_ref=ref.at[src], dst_ref=ref.at[dst],
                send_sem=x_send.at[i], recv_sem=x_recv.at[i],
                device_id=(dev[to],), device_id_type=MESH,
            )
        )
        moves[-1].start()

    thresh = (th_ref[0] - 2).astype(F32)

    def open_across(t):
        for g in range(WORDS):
            A[0, t, 32 * g:32 * g + 32, :] = unpack(acr[t, g:g + 1, :]).astype(F32).astype(F8)

    def open_within(t):
        for g in range(WORDS):
            r = lax.broadcasted_iota(I32, (32, TILE), 0) + 32 * g
            c = lax.broadcasted_iota(I32, (32, TILE), 1)
            U[32 * g:32 * g + 32, :] = jnp.where(c > r, unpack(wit[t, g:g + 1, :]), 0).astype(F32)
        u = U[...]
        W[0, t] = (u + u.T).astype(F8)

    def keep(x, old):
        return jnp.where(x >= thresh, old.astype(F32), 0.0)

    def edges(w, a):
        s = jnp.sum(w, axis=0, keepdims=True) * 0.5 + jnp.sum(a, axis=0, keepdims=True)
        return jnp.sum(s, axis=1, keepdims=True)

    def inside(s, j):
        return (
            dot_tn(A[s, j], A[s, j]) + dot(W[s, j], W[s, j]) + dot_nt(A[s, j + 1], A[s, j + 1])
        )

    def between(s, j):
        return dot(W[s, j], A[s, j + 1]) + dot(A[s, j + 1], W[s, j + 1])

    open_across(2)
    open_within(1)
    a = A[0, 2]
    w = W[0, 1]
    total = [edges(w.astype(F32), a.astype(F32))]
    Pw[...] = dot(w, w) + dot_nt(a, a)
    Qa[...] = dot(w, a)

    def from_left():
        for i in (0, 2, 4):
            moves[i].wait_recv()
        open_across(1)
        open_within(0)
        open_across(0)
        W[1, 1] = keep(dot_tn(A[0, 1], A[0, 1]) + Pw[...], W[0, 1]).astype(F8)
        A[1, 1] = keep(between(0, 0), A[0, 1]).astype(F8)
        W[1, 0] = keep(inside(0, 0), W[0, 0]).astype(F8)

    def from_right():
        for i in (1, 3, 5):
            moves[i].wait_recv()
        open_within(2)
        open_across(3)
        open_within(3)
        A[1, 2] = keep(dot(A[0, 2], W[0, 2]) + Qa[...], A[0, 2]).astype(F8)
        W[1, 2] = keep(inside(0, 2), W[0, 2]).astype(F8)
        A[1, 3] = keep(between(0, 2), A[0, 3]).astype(F8)

    last_chip = lax.rem(lax.div(chip, XAX[0]), XAX[1]) == XAX[1] - 1

    @pl.when(last_chip)
    def _():
        from_left()
        from_right()

    @pl.when(jnp.logical_not(last_chip))
    def _():
        from_right()
        from_left()

    total.append(edges(W[1, 1].astype(F32), A[1, 2].astype(F32)))
    A[0, 1] = keep(between(1, 0), A[1, 1]).astype(F8)
    W[0, 2] = keep(inside(1, 2), W[1, 2]).astype(F8)
    w = keep(inside(1, 1), W[1, 1])
    W[0, 1] = w.astype(F8)
    a = keep(between(1, 1), A[1, 2])
    A[0, 2] = a.astype(F8)
    total.append(edges(w, a))

    x = inside(0, 1)
    sup[:, :TILE] = x
    w = keep(x, W[0, 1])
    y = between(0, 1)
    sup[:, TILE:] = y
    a = keep(y, A[0, 2])
    total.append(edges(w, a))

    lane = lax.broadcasted_iota(I32, (1, 128), 1)
    acc = jnp.zeros((1, 128), I32)
    for i in range(3):
        lost = (total[i] - total[i + 1]).astype(I32)
        acc = jnp.where(lane == i, lost, acc)
    near, wide = len(gather), len(spread)
    sbuf[0:1, :] = acc
    buf1[2 * near - 1:2 * near, :] = acc

    def send(stage, buf, row, count, device):
        return pltpu.make_async_remote_copy(
            src_ref=(sbuf if count == 1 else buf).at[pl.ds(stage if count == 1 else 0, count)],
            dst_ref=buf.at[pl.ds(row, count)],
            send_sem=r_send.at[stage], recv_sem=r_recv.at[stage],
            device_id=(device,), device_id_type=MESH,
        )

    @pl.when(core == 0)
    def _():
        for k in range(near - 1, 0, -1):
            send(0, buf1, 2 * k - 2, 1, gather[k] + 1).start()
        send(0, buf1, 2 * near - 2, 1, mate).start()

    @pl.when(core == 1)
    def _():
        for k in range(near - 1, 0, -1):
            send(0, buf1, 2 * k - 1, 1, gather[k] + 1).start()

    sup[:, :TILE] = sup[:, :TILE] * jnp.where(
        sup[:, :TILE] >= thresh, W[0, 1].astype(F32), 0.0)
    sup[:, TILE:] = sup[:, TILE:] * jnp.where(
        sup[:, TILE:] >= thresh, A[0, 2].astype(F32), 0.0)
    for c in moves:
        c.wait_send()

    @pl.when(core == 0)
    def _():
        send(0, buf1, 0, near, mate).wait_send()
        send(2, buf3, 0, 1, mate).wait_recv()

    @pl.when(core == 1)
    def _():
        send(0, buf1, 0, 2 * near - 1, mate).wait_recv()
        part = jnp.sum(buf1[...], axis=0, keepdims=True)
        sbuf[1:2, :] = part
        buf2[wide - 1:wide, :] = part
        for k in range(wide - 1, 0, -1):
            send(1, buf2, k - 1, 1, spread[k] + 1).start()
        send(0, buf1, 0, near - 1, mate).wait_send()
        send(1, buf2, 0, wide - 1, mate).wait_recv()
        whole = jnp.sum(buf2[...], axis=0, keepdims=True)
        sbuf[2:3, :] = whole
        send(2, buf3, 0, 1, mate).start()
        buf3[0:1, :] = whole
        send(1, buf2, 0, wide - 1, mate).wait_send()
        send(2, buf3, 0, 1, mate).wait_send()

    cnt_ref[...] = buf3[0, :3]


def write_kernel(sup, cnt, out, counts, sem):
    copies = [
        pltpu.make_async_copy(sup.at[pl.ds(64 * i, 64)], out.at[pl.ds(64 * i, 64)], sem.at[i])
        for i in range(8)
    ] + [pltpu.make_async_copy(cnt, counts, sem.at[8])]
    for c in copies:
        c.start()
    for c in copies:
        c.wait()


def group_size(axes):
    size = 1
    for _, s in axes:
        size *= s
    return size


def on_device(adj_diag, adj_right, alive_diag, alive_right, truss_k):
    n = lax.axis_size("rows")
    vmem = pl.BlockSpec(memory_space=pltpu.VMEM)
    smem = pl.BlockSpec(memory_space=pltpu.SMEM)
    hbm = pl.BlockSpec(memory_space=pl.ANY)
    tiles = [
        pltpu.with_memory_space_constraint(x, pltpu.HBM)
        for x in (adj_diag, adj_right, alive_diag, alive_right)
    ]
    support, counts = pl.pallas_call(
        lambda *refs: peel_kernel(n, *refs),
        out_shape=(
            pltpu.VMEM((TILE, 2 * TILE), F32),
            pltpu.VMEM((3,), I32),
        ),
        in_specs=[pl.BlockSpec(memory_space=pltpu.HBM)] * 4 + [smem],
        out_specs=[vmem, vmem],
        scratch_shapes=[
            pltpu.VMEM((4, WORDS, TILE), I32),
            pltpu.VMEM((HALF, WORDS, TILE), I32),
            pltpu.VMEM((HALF, WORDS, TILE), I32),
            pltpu.VMEM((2, HALF, TILE, TILE), F8),
            pltpu.VMEM((2, HALF, TILE, TILE), F8),
            pltpu.VMEM((TILE, TILE), F32),
            pltpu.VMEM((TILE, TILE), F32),
            pltpu.VMEM((TILE, TILE), F32),
            pltpu.VMEM((3, 128), I32),
            pltpu.VMEM((2 * group_size(GATHER), 128), I32),
            pltpu.VMEM((group_size(SPREAD), 128), I32),
            pltpu.VMEM((1, 128), I32),
            pltpu.SemaphoreType.DMA((4,)),
            pltpu.SemaphoreType.DMA((6,)),
            pltpu.SemaphoreType.DMA((6,)),
            pltpu.SemaphoreType.DMA((3,)),
            pltpu.SemaphoreType.DMA((3,)),
        ],
        compiler_params=pltpu.CompilerParams(
            collective_id=0, has_side_effects=True, vmem_limit_bytes=40 * 2**20
        ),
        name="peel",
    )(*tiles, truss_k)
    return pl.pallas_call(
        write_kernel,
        out_shape=(
            jax.ShapeDtypeStruct((TILE, 2 * TILE), F32),
            jax.ShapeDtypeStruct((3,), I32),
        ),
        in_specs=[vmem, vmem],
        out_specs=[hbm, hbm],
        scratch_shapes=[pltpu.SemaphoreType.DMA((9,))],
        compiler_params=pltpu.CompilerParams(vmem_limit_bytes=4 * 2**20),
        name="write",
    )(support, counts)


def solution(mesh):
    rows = P("rows", None)
    return jax.shard_map(
        on_device, mesh=mesh, in_specs=(rows, rows, rows, rows, P(None)),
        out_specs=(rows, P(None)), check_vma=False,
    )
```

```python
import jax
import jax.numpy as jnp
from jax import lax
from jax.experimental import pallas as pl
from jax.experimental.pallas import tpu as pltpu
from jax.sharding import PartitionSpec as P

TILE = 512
WORDS = TILE // 32
HALF = 4
F8 = jnp.float8_e4m3fn
F32 = jnp.float32
I32 = jnp.int32
MESH = pl.DeviceIdType.MESH
XAX, YAX, ZAX = (2, 4), (8, 8), (64, 8)
GATHER = (YAX,)
SPREAD = (XAX, ZAX)

PIECES = [(q, c) for q in range(4) for c in range(q, 4)]


def chips_of(chip, axes):
    ids = [chip]
    for stride, size in axes:
        pos = lax.rem(lax.div(chip, stride), size)
        ids = [
            base + (lax.rem(pos + k, size) - pos) * stride if k else base
            for base in ids for k in range(size)
        ]
    return ids


def dot(a, b):
    return jnp.dot(a, b, preferred_element_type=F32)


def dot_tn(a, b):
    return lax.dot_general(a, b, (((0,), (0,)), ((), ())), preferred_element_type=F32)


def dot_nt(a, b):
    return lax.dot_general(a, b, (((1,), (1,)), ((), ())), preferred_element_type=F32)


def unpack(words):
    bit = lax.broadcasted_iota(I32, (32, words.shape[1]), 0)
    return (words >> bit) & 1


def peel_kernel(
    n, ad, ar, ld, lr, th_ref, sup, cnt_ref,
    raw, acr, wit, A, W, Pw, Qa, sbuf, buf1, buf2, buf3,
    in_sem, x_send, x_recv, r_send, r_recv,
):
    me = lax.axis_index("rows")
    core = lax.rem(me, 2)
    chip = me - core
    mate = chip + 1 - core
    gather = chips_of(chip, GATHER)
    spread = chips_of(chip, SPREAD)
    place = lax.rem(lax.div(chip, XAX[0]), XAX[1])
    plane_no = lax.div(chip, ZAX[0])
    first = [chip - plane_no * ZAX[0] + (k - place) * XAX[0] for k in range(XAX[1])]
    early_even = jnp.logical_and(core == 0, plane_no == 0)
    late_even = jnp.logical_and(core == 0, plane_no > 0)
    dev = {k: lax.rem(me + k + n, n) for k in (-2, -1, 1, 2)}

    loads = [
        pltpu.make_async_copy(src, raw.at[i], in_sem.at[i])
        for i, src in enumerate((ar, lr, ad, ld))
    ]
    for c in loads:
        c.start()

    barrier = pltpu.get_barrier_semaphore()

    def signal(device):
        pl.semaphore_signal(barrier, inc=1, device_id=(device,), device_id_type=MESH)

    for k in dev:
        signal(dev[k])

    near, wide = len(gather), len(spread)
    deep = SPREAD[1][1]
    line = sorted(range(1, near), key=lambda k: abs(k - near // 2))
    signal(mate)
    for k in line:
        signal(gather[k] + 1)

        @pl.when(core == 1)
        def _():
            signal(gather[k])

    @pl.when(core == 1)
    def _():
        for k in sorted(
            range(1, wide),
            key=lambda k: abs(k % deep - deep // 2) + abs(k // deep - wide // deep // 2),
        ):
            signal(spread[k] + 1)
        for c in first:
            signal(c)

    @pl.when(early_even)
    def _():
        for c in spread:
            signal(c + 1)

    loads[0].wait()
    loads[1].wait()
    acr[2] = raw[0] & raw[1]
    loads[2].wait()
    loads[3].wait()
    for h, (q, c) in enumerate(PIECES):
        row, lane = slice(4 * q, 4 * q + 4), slice(128 * c, 128 * c + 128)
        at = slice(4 * (h % 2), 4 * (h % 2) + 4)
        wit[1, h // 2, at, :] = raw[2, row, lane] & raw[3, row, lane]
    even_count = 4 + near

    @pl.when(late_even)
    def _():
        pl.semaphore_wait(barrier, even_count)

    @pl.when(early_even)
    def _():
        pl.semaphore_wait(barrier, even_count + wide)

    @pl.when(core == 1)
    def _():
        pl.semaphore_wait(barrier, even_count + near - 1 + wide - 1 + len(first))

    plan = (
        (acr, 2, 1, 1), (wit, 1, -1, 2), (wit, 1, 1, 0), (acr, 2, -1, 3),
        (acr, 2, 2, 0), (wit, 1, -2, 3),
    )
    moves = []
    for i, (ref, src, to, dst) in enumerate(plan):
        moves.append(
            pltpu.make_async_remote_copy(
                src_ref=ref.at[src], dst_ref=ref.at[dst],
                send_sem=x_send.at[i], recv_sem=x_recv.at[i],
                device_id=(dev[to],), device_id_type=MESH,
            )
        )
    for c in moves[:4]:
        c.start()

    thresh = (th_ref[0] - 2).astype(F32)

    def open_across(t):
        for g in range(WORDS):
            A[0, t, 32 * g:32 * g + 32, :] = unpack(acr[t, g:g + 1, :]).astype(F32).astype(F8)

    def open_within(t):
        row = lax.broadcasted_iota(I32, (128, 128), 0)
        col = lax.broadcasted_iota(I32, (128, 128), 1)
        for h, (q, c) in enumerate(PIECES):
            first = 4 * (h % 2)
            block = jnp.concatenate(
                [unpack(wit[t, h // 2, first + g:first + g + 1, :]) for g in range(4)], axis=0
            )
            if q == c:
                block = jnp.where(col > row, block, 0)
            block = block.astype(F32)
            flip = block.T
            up, across = pl.ds(128 * q, 128), pl.ds(128 * c, 128)
            if q == c:
                W[0, t, up, up] = (block + flip).astype(F8)
            else:
                W[0, t, up, across] = block.astype(F8)
                W[0, t, across, up] = flip.astype(F8)

    def keep(x, old):
        return jnp.where(x >= thresh, old.astype(F32), 0.0)

    def edges(w, a):
        s = jnp.sum(w, axis=0, keepdims=True) * 0.5 + jnp.sum(a, axis=0, keepdims=True)
        return jnp.sum(s, axis=1, keepdims=True)

    def inside(s, j):
        return (
            dot_tn(A[s, j], A[s, j]) + dot(W[s, j], W[s, j]) + dot_nt(A[s, j + 1], A[s, j + 1])
        )

    def between(s, j):
        return dot(W[s, j], A[s, j + 1]) + dot(A[s, j + 1], W[s, j + 1])

    open_across(2)
    open_within(1)
    a = A[0, 2]
    w = W[0, 1]
    total = [edges(w.astype(F32), a.astype(F32))]
    Pw[...] = dot(w, w) + dot_nt(a, a)
    Qa[...] = dot(w, a)

    for c in moves[4:]:
        c.start()

    def near_left():
        moves[0].wait_recv()
        moves[2].wait_recv()
        open_across(1)
        open_within(0)
        W[1, 1] = keep(dot_tn(A[0, 1], A[0, 1]) + Pw[...], W[0, 1]).astype(F8)
        A[1, 1] = keep(between(0, 0), A[0, 1]).astype(F8)

    def far_left():
        moves[4].wait_recv()
        open_across(0)
        W[1, 0] = keep(inside(0, 0), W[0, 0]).astype(F8)

    def near_right():
        moves[1].wait_recv()
        moves[3].wait_recv()
        open_within(2)
        open_across(3)
        A[1, 2] = keep(dot(A[0, 2], W[0, 2]) + Qa[...], A[0, 2]).astype(F8)
        W[1, 2] = keep(inside(0, 2), W[0, 2]).astype(F8)

    def far_right():
        moves[5].wait_recv()
        open_within(3)
        A[1, 3] = keep(between(0, 2), A[0, 3]).astype(F8)

    def second_left():
        A[0, 1] = keep(between(1, 0), A[1, 1]).astype(F8)

    def second_right():
        W[0, 2] = keep(inside(1, 2), W[1, 2]).astype(F8)

    @pl.when(place == XAX[1] - 1)
    def _():
        near_left()
        far_left()
        second_left()
        near_right()
        far_right()
        second_right()

    @pl.when(place == 0)
    def _():
        near_right()
        far_right()
        second_right()
        near_left()
        far_left()
        second_left()

    @pl.when(jnp.logical_and(place > 0, place < XAX[1] - 1))
    def _():
        near_right()
        near_left()
        far_right()
        far_left()
        second_right()
        second_left()

    total.append(edges(W[1, 1].astype(F32), A[1, 2].astype(F32)))
    w = keep(inside(1, 1), W[1, 1])
    W[0, 1] = w.astype(F8)
    a = keep(between(1, 1), A[1, 2])
    A[0, 2] = a.astype(F8)
    total.append(edges(w, a))

    x = inside(0, 1)
    sup[:, :TILE] = x
    w = keep(x, W[0, 1])
    y = between(0, 1)
    sup[:, TILE:] = y
    a = keep(y, A[0, 2])
    total.append(edges(w, a))

    lane = lax.broadcasted_iota(I32, (1, 128), 1)
    acc = jnp.zeros((1, 128), I32)
    for i in range(3):
        lost = (total[i] - total[i + 1]).astype(I32)
        acc = jnp.where(lane == i, lost, acc)
    plane = sorted(range(1, wide), key=lambda k: (k % deep - 2) % deep)
    sbuf[0:1, :] = acc
    buf1[2 * near - 1:2 * near, :] = acc

    def send(stage, buf, row, count, device):
        return pltpu.make_async_remote_copy(
            src_ref=(sbuf if count == 1 else buf).at[pl.ds(stage if count == 1 else 0, count)],
            dst_ref=buf.at[pl.ds(row, count)],
            send_sem=r_send.at[stage], recv_sem=r_recv.at[stage],
            device_id=(device,), device_id_type=MESH,
        )

    @pl.when(core == 0)
    def _():
        for k in line:
            send(0, buf1, 2 * k - 2, 1, gather[k] + 1).start()
        send(0, buf1, 2 * near - 2, 1, mate).start()

    @pl.when(core == 1)
    def _():
        for k in line:
            send(0, buf1, 2 * k - 1, 1, gather[k] + 1).start()

    sup[:, :TILE] = sup[:, :TILE] * jnp.where(
        sup[:, :TILE] >= thresh, W[0, 1].astype(F32), 0.0)
    sup[:, TILE:] = sup[:, TILE:] * jnp.where(
        sup[:, TILE:] >= thresh, A[0, 2].astype(F32), 0.0)
    for c in moves:
        c.wait_send()

    @pl.when(core == 0)
    def _():
        send(0, buf1, 0, near, mate).wait_send()

    @pl.when(late_even)
    def _():
        send(2, buf3, 0, 1, mate).wait_recv()
        cnt_ref[...] = buf3[0, :3]

    @pl.when(early_even)
    def _():
        send(1, buf2, 0, wide, mate).wait_recv()
        cnt_ref[...] = jnp.sum(buf2[...], axis=0)[:3]

    @pl.when(core == 1)
    def _():
        send(0, buf1, 0, 2 * near - 1, mate).wait_recv()
        part = jnp.sum(buf1[...], axis=0, keepdims=True)
        sbuf[1:2, :] = part
        buf2[wide - 1:wide, :] = part
        for k in plane:
            send(1, buf2, k - 1, 1, spread[k] + 1).start()
        for c in first:
            send(1, buf2, plane_no * XAX[1] + place, 1, c).start()
        send(0, buf1, 0, near - 1, mate).wait_send()
        send(1, buf2, 0, wide - 1, mate).wait_recv()
        whole = jnp.sum(buf2[...], axis=0, keepdims=True)
        cnt_ref[...] = whole[0, :3]

        @pl.when(plane_no > 0)
        def _():
            sbuf[2:3, :] = whole
            send(2, buf3, 0, 1, mate).start()
            send(2, buf3, 0, 1, mate).wait_send()

        send(1, buf2, 0, wide - 1, mate).wait_send()
        send(1, buf2, 0, len(first), mate).wait_send()


def write_kernel(sup, cnt, out, counts, sem):
    copies = [
        pltpu.make_async_copy(sup.at[pl.ds(64 * i, 64)], out.at[pl.ds(64 * i, 64)], sem.at[i])
        for i in range(8)
    ] + [pltpu.make_async_copy(cnt, counts, sem.at[8])]
    for c in copies:
        c.start()
    for c in copies:
        c.wait()


def group_size(axes):
    size = 1
    for _, s in axes:
        size *= s
    return size


def on_device(adj_diag, adj_right, alive_diag, alive_right, truss_k):
    n = lax.axis_size("rows")
    vmem = pl.BlockSpec(memory_space=pltpu.VMEM)
    smem = pl.BlockSpec(memory_space=pltpu.SMEM)
    hbm = pl.BlockSpec(memory_space=pl.ANY)
    tiles = [
        pltpu.with_memory_space_constraint(x, pltpu.HBM)
        for x in (adj_diag, adj_right, alive_diag, alive_right)
    ]
    support, counts = pl.pallas_call(
        lambda *refs: peel_kernel(n, *refs),
        out_shape=(
            pltpu.VMEM((TILE, 2 * TILE), F32),
            pltpu.VMEM((3,), I32),
        ),
        in_specs=[pl.BlockSpec(memory_space=pltpu.HBM)] * 4 + [smem],
        out_specs=[vmem, vmem],
        scratch_shapes=[
            pltpu.VMEM((4, WORDS, TILE), I32),
            pltpu.VMEM((HALF, WORDS, TILE), I32),
            pltpu.VMEM((HALF, len(PIECES) // 2, 8, 128), I32),
            pltpu.VMEM((2, HALF, TILE, TILE), F8),
            pltpu.VMEM((2, HALF, TILE, TILE), F8),
            pltpu.VMEM((TILE, TILE), F32),
            pltpu.VMEM((TILE, TILE), F32),
            pltpu.VMEM((3, 128), I32),
            pltpu.VMEM((2 * group_size(GATHER), 128), I32),
            pltpu.VMEM((group_size(SPREAD), 128), I32),
            pltpu.VMEM((1, 128), I32),
            pltpu.SemaphoreType.DMA((4,)),
            pltpu.SemaphoreType.DMA((6,)),
            pltpu.SemaphoreType.DMA((6,)),
            pltpu.SemaphoreType.DMA((3,)),
            pltpu.SemaphoreType.DMA((3,)),
        ],
        compiler_params=pltpu.CompilerParams(
            collective_id=0, has_side_effects=True, vmem_limit_bytes=40 * 2**20
        ),
        name="peel",
    )(*tiles, truss_k)
    return pl.pallas_call(
        write_kernel,
        out_shape=(
            jax.ShapeDtypeStruct((TILE, 2 * TILE), F32),
            jax.ShapeDtypeStruct((3,), I32),
        ),
        in_specs=[vmem, vmem],
        out_specs=[hbm, hbm],
        scratch_shapes=[pltpu.SemaphoreType.DMA((9,))],
        compiler_params=pltpu.CompilerParams(vmem_limit_bytes=4 * 2**20),
        name="write",
    )(support, counts)


def solution(mesh):
    rows = P("rows", None)
    return jax.shard_map(
        on_device, mesh=mesh, in_specs=(rows, rows, rows, rows, P(None)),
        out_specs=(rows, P(None)), check_vma=False,
    )
```

```python
import jax
import jax.numpy as jnp
from jax import lax
from jax.experimental import pallas as pl
from jax.experimental.pallas import tpu as pltpu
from jax.sharding import PartitionSpec as P

TILE = 512
WORDS = TILE // 32
HALF = 4
F8 = jnp.float8_e4m3fn
F32 = jnp.float32
I32 = jnp.int32
MESH = pl.DeviceIdType.MESH
XAX, YAX, ZAX = (2, 4), (8, 8), (64, 8)
GATHER = (XAX,)
SPREAD = (YAX, ZAX)

PIECES = [(q, c) for q in range(4) for c in range(q, 4)]


def chips_of(chip, axes):
    ids = [chip]
    for stride, size in axes:
        pos = lax.rem(lax.div(chip, stride), size)
        ids = [
            base + (lax.rem(pos + k, size) - pos) * stride if k else base
            for base in ids for k in range(size)
        ]
    return ids


def dot(a, b):
    return jnp.dot(a, b, preferred_element_type=F32)


def dot_tn(a, b):
    return lax.dot_general(a, b, (((0,), (0,)), ((), ())), preferred_element_type=F32)


def dot_nt(a, b):
    return lax.dot_general(a, b, (((1,), (1,)), ((), ())), preferred_element_type=F32)


def unpack(words):
    bit = lax.broadcasted_iota(I32, (32, words.shape[1]), 0)
    return (words >> bit) & 1


def peel_kernel(
    n, ad, ar, ld, lr, th_ref, sup, cnt_ref,
    raw, acr, wit, A, W, Pw, Qa, sbuf, buf1, buf2, buf3,
    in_sem, x_send, x_recv, r_send, r_recv,
):
    me = lax.axis_index("rows")
    core = lax.rem(me, 2)
    chip = me - core
    mate = chip + 1 - core
    gather = chips_of(chip, GATHER)
    spread = chips_of(chip, SPREAD)
    place = lax.rem(lax.div(chip, XAX[0]), XAX[1])
    plane_no = lax.div(chip, ZAX[0])
    outer, length = SPREAD[0]
    spot = lax.rem(lax.div(chip, outer), length)
    first = [chip - plane_no * ZAX[0] + (k - spot) * outer for k in range(length)]
    early_even = jnp.logical_and(core == 0, plane_no == 0)
    late_even = jnp.logical_and(core == 0, plane_no > 0)
    dev = {k: lax.rem(me + k + n, n) for k in (-2, -1, 1, 2)}

    loads = [
        pltpu.make_async_copy(src, raw.at[i], in_sem.at[i])
        for i, src in enumerate((ar, lr, ad, ld))
    ]
    for c in loads:
        c.start()

    barrier = pltpu.get_barrier_semaphore()

    def signal(device):
        pl.semaphore_signal(barrier, inc=1, device_id=(device,), device_id_type=MESH)

    for k in dev:
        signal(dev[k])

    near, wide = len(gather), len(spread)
    deep = SPREAD[1][1]
    line = sorted(range(1, near), key=lambda k: abs(k - near // 2))

    @pl.when(core == 1)
    def _():
        for k in line:
            signal(gather[k] + 1)
            signal(gather[k])
        for k in sorted(
            range(1, wide),
            key=lambda k: abs(k % deep - deep // 2) + abs(k // deep - wide // deep // 2),
        ):
            signal(spread[k] + 1)
        signal(mate)

    @pl.when(early_even)
    def _():
        for c in spread:
            signal(c + 1)

    @pl.when(late_even)
    def _():
        signal(mate)

    loads[0].wait()
    loads[1].wait()
    acr[2] = raw[0] & raw[1]
    loads[2].wait()
    loads[3].wait()
    for h, (q, c) in enumerate(PIECES):
        row, lane = slice(4 * q, 4 * q + 4), slice(128 * c, 128 * c + 128)
        at = slice(4 * (h % 2), 4 * (h % 2) + 4)
        wit[1, h // 2, at, :] = raw[2, row, lane] & raw[3, row, lane]
    @pl.when(core == 0)
    def _():
        pl.semaphore_wait(barrier, 4 + near)

    @pl.when(jnp.logical_and(core == 1, plane_no > 0))
    def _():
        pl.semaphore_wait(barrier, 4 + near - 1 + wide - 1 + len(first) + 1)

    @pl.when(jnp.logical_and(core == 1, plane_no == 0))
    def _():
        pl.semaphore_wait(barrier, 4 + near - 1 + wide - 1 + len(first))

    plan = (
        (acr, 2, 1, 1), (wit, 1, -1, 2), (wit, 1, 1, 0), (acr, 2, -1, 3),
        (acr, 2, 2, 0), (wit, 1, -2, 3),
    )
    moves = []
    for i, (ref, src, to, dst) in enumerate(plan):
        moves.append(
            pltpu.make_async_remote_copy(
                src_ref=ref.at[src], dst_ref=ref.at[dst],
                send_sem=x_send.at[i], recv_sem=x_recv.at[i],
                device_id=(dev[to],), device_id_type=MESH,
            )
        )
    for c in moves[:4]:
        c.start()

    thresh = (th_ref[0] - 2).astype(F32)

    def open_across(t):
        for g in range(WORDS):
            A[0, t, 32 * g:32 * g + 32, :] = unpack(acr[t, g:g + 1, :]).astype(F32).astype(F8)

    def open_within(t):
        row = lax.broadcasted_iota(I32, (128, 128), 0)
        col = lax.broadcasted_iota(I32, (128, 128), 1)
        for h, (q, c) in enumerate(PIECES):
            first = 4 * (h % 2)
            block = jnp.concatenate(
                [unpack(wit[t, h // 2, first + g:first + g + 1, :]) for g in range(4)], axis=0
            )
            if q == c:
                block = jnp.where(col > row, block, 0)
            block = block.astype(F32)
            flip = block.T
            up, across = pl.ds(128 * q, 128), pl.ds(128 * c, 128)
            if q == c:
                W[0, t, up, up] = (block + flip).astype(F8)
            else:
                W[0, t, up, across] = block.astype(F8)
                W[0, t, across, up] = flip.astype(F8)

    def keep(x, old):
        return jnp.where(x >= thresh, old.astype(F32), 0.0)

    def edges(w, a):
        s = jnp.sum(w, axis=0, keepdims=True) * 0.5 + jnp.sum(a, axis=0, keepdims=True)
        return jnp.sum(s, axis=1, keepdims=True)

    def inside(s, j):
        return (
            dot_tn(A[s, j], A[s, j]) + dot(W[s, j], W[s, j]) + dot_nt(A[s, j + 1], A[s, j + 1])
        )

    def between(s, j):
        return dot(W[s, j], A[s, j + 1]) + dot(A[s, j + 1], W[s, j + 1])

    open_across(2)
    open_within(1)
    a = A[0, 2]
    w = W[0, 1]
    total = [edges(w.astype(F32), a.astype(F32))]
    Pw[...] = dot(w, w) + dot_nt(a, a)
    Qa[...] = dot(w, a)

    for c in moves[4:]:
        c.start()

    def near_left():
        moves[0].wait_recv()
        moves[2].wait_recv()
        open_across(1)
        open_within(0)
        W[1, 1] = keep(dot_tn(A[0, 1], A[0, 1]) + Pw[...], W[0, 1]).astype(F8)
        A[1, 1] = keep(between(0, 0), A[0, 1]).astype(F8)

    def far_left():
        moves[4].wait_recv()
        open_across(0)
        W[1, 0] = keep(inside(0, 0), W[0, 0]).astype(F8)

    def near_right():
        moves[1].wait_recv()
        moves[3].wait_recv()
        open_within(2)
        open_across(3)
        A[1, 2] = keep(dot(A[0, 2], W[0, 2]) + Qa[...], A[0, 2]).astype(F8)
        W[1, 2] = keep(inside(0, 2), W[0, 2]).astype(F8)

    def far_right():
        moves[5].wait_recv()
        open_within(3)
        A[1, 3] = keep(between(0, 2), A[0, 3]).astype(F8)

    def second_left():
        A[0, 1] = keep(between(1, 0), A[1, 1]).astype(F8)

    def second_right():
        W[0, 2] = keep(inside(1, 2), W[1, 2]).astype(F8)

    @pl.when(place == XAX[1] - 1)
    def _():
        near_left()
        far_left()
        second_left()
        near_right()
        far_right()
        second_right()

    @pl.when(place == 0)
    def _():
        near_right()
        far_right()
        second_right()
        near_left()
        far_left()
        second_left()

    @pl.when(jnp.logical_and(place > 0, place < XAX[1] - 1))
    def _():
        near_right()
        near_left()
        far_right()
        far_left()
        second_right()
        second_left()

    total.append(edges(W[1, 1].astype(F32), A[1, 2].astype(F32)))
    w = keep(inside(1, 1), W[1, 1])
    W[0, 1] = w.astype(F8)
    a = keep(between(1, 1), A[1, 2])
    A[0, 2] = a.astype(F8)
    total.append(edges(w, a))

    x = inside(0, 1)
    sup[:, :TILE] = x
    w = keep(x, W[0, 1])
    y = between(0, 1)
    sup[:, TILE:] = y
    a = keep(y, A[0, 2])
    total.append(edges(w, a))

    lane = lax.broadcasted_iota(I32, (1, 128), 1)
    acc = jnp.zeros((1, 128), I32)
    for i in range(3):
        lost = (total[i] - total[i + 1]).astype(I32)
        acc = jnp.where(lane == i, lost, acc)
    plane = sorted(range(1, wide), key=lambda k: ((k % deep - 1) % deep, abs(k // deep - length // 2)))
    sbuf[0:1, :] = acc
    buf1[2 * near - 1:2 * near, :] = acc

    def send(stage, buf, row, count, device):
        return pltpu.make_async_remote_copy(
            src_ref=(sbuf if count == 1 else buf).at[pl.ds(stage if count == 1 else 0, count)],
            dst_ref=buf.at[pl.ds(row, count)],
            send_sem=r_send.at[stage], recv_sem=r_recv.at[stage],
            device_id=(device,), device_id_type=MESH,
        )

    @pl.when(core == 0)
    def _():
        for k in line:
            send(0, buf1, 2 * k - 2, 1, gather[k] + 1).start()
        send(0, buf1, 2 * near - 2, 1, mate).start()

    @pl.when(core == 1)
    def _():
        for k in line:
            send(0, buf1, 2 * k - 1, 1, gather[k] + 1).start()

    sup[:, :TILE] = sup[:, :TILE] * jnp.where(
        sup[:, :TILE] >= thresh, W[0, 1].astype(F32), 0.0)
    sup[:, TILE:] = sup[:, TILE:] * jnp.where(
        sup[:, TILE:] >= thresh, A[0, 2].astype(F32), 0.0)
    for c in moves:
        c.wait_send()

    @pl.when(core == 0)
    def _():
        send(0, buf1, 0, near, mate).wait_send()

    @pl.when(late_even)
    def _():
        send(2, buf3, 0, 1, mate).wait_recv()
        cnt_ref[...] = buf3[0, :3]

    @pl.when(early_even)
    def _():
        send(1, buf2, 0, wide, mate).wait_recv()
        cnt_ref[...] = jnp.sum(buf2[...], axis=0)[:3]

    @pl.when(core == 1)
    def _():
        send(0, buf1, 0, 2 * near - 1, mate).wait_recv()
        part = jnp.sum(buf1[...], axis=0, keepdims=True)
        sbuf[1:2, :] = part
        buf2[wide - 1:wide, :] = part
        for k in plane:
            send(1, buf2, k - 1, 1, spread[k] + 1).start()
        for c in first:
            send(1, buf2, plane_no * length + spot, 1, c).start()
        send(0, buf1, 0, near - 1, mate).wait_send()
        send(1, buf2, 0, wide - 1, mate).wait_recv()
        whole = jnp.sum(buf2[...], axis=0, keepdims=True)
        cnt_ref[...] = whole[0, :3]

        @pl.when(plane_no > 0)
        def _():
            sbuf[2:3, :] = whole
            send(2, buf3, 0, 1, mate).start()
            send(2, buf3, 0, 1, mate).wait_send()

        send(1, buf2, 0, wide - 1, mate).wait_send()
        send(1, buf2, 0, len(first), mate).wait_send()


def write_kernel(sup, cnt, out, counts, sem):
    copies = [
        pltpu.make_async_copy(sup.at[pl.ds(64 * i, 64)], out.at[pl.ds(64 * i, 64)], sem.at[i])
        for i in range(8)
    ] + [pltpu.make_async_copy(cnt, counts, sem.at[8])]
    for c in copies:
        c.start()
    for c in copies:
        c.wait()


def group_size(axes):
    size = 1
    for _, s in axes:
        size *= s
    return size


def on_device(adj_diag, adj_right, alive_diag, alive_right, truss_k):
    n = lax.axis_size("rows")
    vmem = pl.BlockSpec(memory_space=pltpu.VMEM)
    smem = pl.BlockSpec(memory_space=pltpu.SMEM)
    hbm = pl.BlockSpec(memory_space=pl.ANY)
    tiles = [
        pltpu.with_memory_space_constraint(x, pltpu.HBM)
        for x in (adj_diag, adj_right, alive_diag, alive_right)
    ]
    support, counts = pl.pallas_call(
        lambda *refs: peel_kernel(n, *refs),
        out_shape=(
            pltpu.VMEM((TILE, 2 * TILE), F32),
            pltpu.VMEM((3,), I32),
        ),
        in_specs=[pl.BlockSpec(memory_space=pltpu.HBM)] * 4 + [smem],
        out_specs=[vmem, vmem],
        scratch_shapes=[
            pltpu.VMEM((4, WORDS, TILE), I32),
            pltpu.VMEM((HALF, WORDS, TILE), I32),
            pltpu.VMEM((HALF, len(PIECES) // 2, 8, 128), I32),
            pltpu.VMEM((2, HALF, TILE, TILE), F8),
            pltpu.VMEM((2, HALF, TILE, TILE), F8),
            pltpu.VMEM((TILE, TILE), F32),
            pltpu.VMEM((TILE, TILE), F32),
            pltpu.VMEM((3, 128), I32),
            pltpu.VMEM((2 * group_size(GATHER), 128), I32),
            pltpu.VMEM((group_size(SPREAD), 128), I32),
            pltpu.VMEM((1, 128), I32),
            pltpu.SemaphoreType.DMA((4,)),
            pltpu.SemaphoreType.DMA((6,)),
            pltpu.SemaphoreType.DMA((6,)),
            pltpu.SemaphoreType.DMA((3,)),
            pltpu.SemaphoreType.DMA((3,)),
        ],
        compiler_params=pltpu.CompilerParams(
            collective_id=0, has_side_effects=True, vmem_limit_bytes=40 * 2**20
        ),
        name="peel",
    )(*tiles, truss_k)
    return pl.pallas_call(
        write_kernel,
        out_shape=(
            jax.ShapeDtypeStruct((TILE, 2 * TILE), F32),
            jax.ShapeDtypeStruct((3,), I32),
        ),
        in_specs=[vmem, vmem],
        out_specs=[hbm, hbm],
        scratch_shapes=[pltpu.SemaphoreType.DMA((9,))],
        compiler_params=pltpu.CompilerParams(vmem_limit_bytes=4 * 2**20),
        name="write",
    )(support, counts)


def solution(mesh):
    rows = P("rows", None)
    return jax.shard_map(
        on_device, mesh=mesh, in_specs=(rows, rows, rows, rows, P(None)),
        out_specs=(rows, P(None)), check_vma=False,
    )
```

```python
import jax
import jax.numpy as jnp
from jax import lax
from jax.experimental import pallas as pl
from jax.experimental.pallas import tpu as pltpu
from jax.sharding import PartitionSpec as P

TILE = 512
WORDS = TILE // 32
HALF = 4
F8 = jnp.float8_e4m3fn
F32 = jnp.float32
I32 = jnp.int32
MESH = pl.DeviceIdType.MESH
XAX, YAX, ZAX = (2, 4), (8, 8), (64, 8)
GATHER = (XAX,)
SPREAD = (YAX, ZAX)

PIECES = [(q, c) for q in range(4) for c in range(q, 4)]


def chips_of(chip, axes):
    ids = [chip]
    for stride, size in axes:
        pos = lax.rem(lax.div(chip, stride), size)
        ids = [
            base + (lax.rem(pos + k, size) - pos) * stride if k else base
            for base in ids for k in range(size)
        ]
    return ids


def dot(a, b):
    return jnp.dot(a, b, preferred_element_type=F32)


def dot_tn(a, b):
    return lax.dot_general(a, b, (((0,), (0,)), ((), ())), preferred_element_type=F32)


def dot_nt(a, b):
    return lax.dot_general(a, b, (((1,), (1,)), ((), ())), preferred_element_type=F32)


def unpack(words):
    bit = lax.broadcasted_iota(I32, (32, words.shape[1]), 0)
    return (words >> bit) & 1


def peel_kernel(
    n, ad, ar, ld, lr, th_ref, sup, cnt_ref,
    raw, acr, wit, A, W, Pw, Qa, sbuf, buf1, buf2, buf3,
    in_sem, x_send, x_recv, r_send, r_recv,
):
    me = lax.axis_index("rows")
    core = lax.rem(me, 2)
    chip = me - core
    mate = chip + 1 - core
    gather = chips_of(chip, GATHER)
    spread = chips_of(chip, SPREAD)
    place = lax.rem(lax.div(chip, XAX[0]), XAX[1])
    plane_no = lax.div(chip, ZAX[0])
    outer, length = SPREAD[0]
    spot = lax.rem(lax.div(chip, outer), length)
    first = [chip - plane_no * ZAX[0] + (k - spot) * outer for k in range(length)]
    early_even = jnp.logical_and(core == 0, plane_no == 0)
    late_even = jnp.logical_and(core == 0, plane_no > 0)
    dev = {k: lax.rem(me + k + n, n) for k in (-2, -1, 1, 2)}

    loads = [
        pltpu.make_async_copy(src, raw.at[i], in_sem.at[i])
        for i, src in enumerate((ar, lr, ad, ld))
    ]
    for c in loads:
        c.start()

    barrier = pltpu.get_barrier_semaphore()

    def signal(device):
        pl.semaphore_signal(barrier, inc=1, device_id=(device,), device_id_type=MESH)

    for k in dev:
        signal(dev[k])

    near, wide = len(gather), len(spread)
    deep = SPREAD[1][1]
    line = sorted(range(1, near), key=lambda k: abs(k - near // 2))

    @pl.when(core == 1)
    def _():
        for k in line:
            signal(gather[k] + 1)
            signal(gather[k])
        for k in sorted(
            range(1, wide),
            key=lambda k: abs(k % deep - deep // 2) + abs(k // deep - wide // deep // 2),
        ):
            signal(spread[k] + 1)
        signal(mate)

    @pl.when(early_even)
    def _():
        for c in spread:
            signal(c + 1)

    @pl.when(late_even)
    def _():
        signal(mate)

    loads[0].wait()
    loads[1].wait()
    acr[2] = raw[0] & raw[1]
    loads[2].wait()
    loads[3].wait()
    for h, (q, c) in enumerate(PIECES):
        row, lane = slice(4 * q, 4 * q + 4), slice(128 * c, 128 * c + 128)
        at = slice(4 * (h % 2), 4 * (h % 2) + 4)
        wit[1, h // 2, at, :] = raw[2, row, lane] & raw[3, row, lane]
    thresh = (th_ref[0] - 2).astype(F32)

    def open_across(t):
        for g in range(WORDS):
            A[0, t, 32 * g:32 * g + 32, :] = unpack(acr[t, g:g + 1, :]).astype(F32).astype(F8)

    def open_within(t):
        row = lax.broadcasted_iota(I32, (128, 128), 0)
        col = lax.broadcasted_iota(I32, (128, 128), 1)
        for h, (q, c) in enumerate(PIECES):
            first = 4 * (h % 2)
            block = jnp.concatenate(
                [unpack(wit[t, h // 2, first + g:first + g + 1, :]) for g in range(4)], axis=0
            )
            if q == c:
                block = jnp.where(col > row, block, 0)
            block = block.astype(F32)
            flip = block.T
            up, across = pl.ds(128 * q, 128), pl.ds(128 * c, 128)
            if q == c:
                W[0, t, up, up] = (block + flip).astype(F8)
            else:
                W[0, t, up, across] = block.astype(F8)
                W[0, t, across, up] = flip.astype(F8)

    def keep(x, old):
        return jnp.where(x >= thresh, old.astype(F32), 0.0)

    def edges(w, a):
        s = jnp.sum(w, axis=0, keepdims=True) * 0.5 + jnp.sum(a, axis=0, keepdims=True)
        return jnp.sum(s, axis=1, keepdims=True)

    def inside(s, j):
        return (
            dot_tn(A[s, j], A[s, j]) + dot(W[s, j], W[s, j]) + dot_nt(A[s, j + 1], A[s, j + 1])
        )

    def between(s, j):
        return dot(W[s, j], A[s, j + 1]) + dot(A[s, j + 1], W[s, j + 1])

    open_across(2)
    open_within(1)
    a = A[0, 2]
    w = W[0, 1]
    total = [edges(w.astype(F32), a.astype(F32))]
    Pw[...] = dot(w, w) + dot_nt(a, a)
    Qa[...] = dot(w, a)

    @pl.when(core == 0)
    def _():
        pl.semaphore_wait(barrier, 4 + near)

    @pl.when(jnp.logical_and(core == 1, plane_no > 0))
    def _():
        pl.semaphore_wait(barrier, 4 + near - 1 + wide - 1 + len(first) + 1)

    @pl.when(jnp.logical_and(core == 1, plane_no == 0))
    def _():
        pl.semaphore_wait(barrier, 4 + near - 1 + wide - 1 + len(first))

    plan = (
        (acr, 2, 1, 1), (wit, 1, -1, 2), (wit, 1, 1, 0), (acr, 2, -1, 3),
        (acr, 2, 2, 0), (wit, 1, -2, 3),
    )
    moves = []
    for i, (ref, src, to, dst) in enumerate(plan):
        moves.append(
            pltpu.make_async_remote_copy(
                src_ref=ref.at[src], dst_ref=ref.at[dst],
                send_sem=x_send.at[i], recv_sem=x_recv.at[i],
                device_id=(dev[to],), device_id_type=MESH,
            )
        )
    for c in moves[:4]:
        c.start()

    for c in moves[4:]:
        c.start()

    def near_left():
        moves[0].wait_recv()
        moves[2].wait_recv()
        open_across(1)
        open_within(0)
        W[1, 1] = keep(dot_tn(A[0, 1], A[0, 1]) + Pw[...], W[0, 1]).astype(F8)
        A[1, 1] = keep(between(0, 0), A[0, 1]).astype(F8)

    def far_left():
        moves[4].wait_recv()
        open_across(0)
        W[1, 0] = keep(inside(0, 0), W[0, 0]).astype(F8)

    def near_right():
        moves[1].wait_recv()
        moves[3].wait_recv()
        open_within(2)
        open_across(3)
        A[1, 2] = keep(dot(A[0, 2], W[0, 2]) + Qa[...], A[0, 2]).astype(F8)
        W[1, 2] = keep(inside(0, 2), W[0, 2]).astype(F8)

    def far_right():
        moves[5].wait_recv()
        open_within(3)
        A[1, 3] = keep(between(0, 2), A[0, 3]).astype(F8)

    def second_left():
        A[0, 1] = keep(between(1, 0), A[1, 1]).astype(F8)

    def second_right():
        W[0, 2] = keep(inside(1, 2), W[1, 2]).astype(F8)

    @pl.when(place == XAX[1] - 1)
    def _():
        near_left()
        far_left()
        second_left()
        near_right()
        far_right()
        second_right()

    @pl.when(place == 0)
    def _():
        near_right()
        far_right()
        second_right()
        near_left()
        far_left()
        second_left()

    @pl.when(jnp.logical_and(place > 0, place < XAX[1] - 1))
    def _():
        near_right()
        near_left()
        far_right()
        far_left()
        second_right()
        second_left()

    total.append(edges(W[1, 1].astype(F32), A[1, 2].astype(F32)))
    w = keep(inside(1, 1), W[1, 1])
    W[0, 1] = w.astype(F8)
    a = keep(between(1, 1), A[1, 2])
    A[0, 2] = a.astype(F8)
    total.append(edges(w, a))

    x = inside(0, 1)
    sup[:, :TILE] = x
    w = keep(x, W[0, 1])
    y = between(0, 1)
    sup[:, TILE:] = y
    a = keep(y, A[0, 2])
    total.append(edges(w, a))

    lane = lax.broadcasted_iota(I32, (1, 128), 1)
    acc = jnp.zeros((1, 128), I32)
    for i in range(3):
        lost = (total[i] - total[i + 1]).astype(I32)
        acc = jnp.where(lane == i, lost, acc)
    plane = sorted(range(1, wide), key=lambda k: ((k % deep - 1) % deep, abs(k // deep - length // 2)))
    sbuf[0:1, :] = acc
    buf1[2 * near - 1:2 * near, :] = acc

    def send(stage, buf, row, count, device):
        return pltpu.make_async_remote_copy(
            src_ref=(sbuf if count == 1 else buf).at[pl.ds(stage if count == 1 else 0, count)],
            dst_ref=buf.at[pl.ds(row, count)],
            send_sem=r_send.at[stage], recv_sem=r_recv.at[stage],
            device_id=(device,), device_id_type=MESH,
        )

    @pl.when(core == 0)
    def _():
        for k in line:
            send(0, buf1, 2 * k - 2, 1, gather[k] + 1).start()
        send(0, buf1, 2 * near - 2, 1, mate).start()

    @pl.when(core == 1)
    def _():
        for k in line:
            send(0, buf1, 2 * k - 1, 1, gather[k] + 1).start()

    sup[:, :TILE] = sup[:, :TILE] * jnp.where(
        sup[:, :TILE] >= thresh, W[0, 1].astype(F32), 0.0)
    sup[:, TILE:] = sup[:, TILE:] * jnp.where(
        sup[:, TILE:] >= thresh, A[0, 2].astype(F32), 0.0)
    for c in moves:
        c.wait_send()

    @pl.when(core == 0)
    def _():
        send(0, buf1, 0, near, mate).wait_send()

    @pl.when(late_even)
    def _():
        send(2, buf3, 0, 1, mate).wait_recv()
        cnt_ref[...] = buf3[0, :3]

    @pl.when(early_even)
    def _():
        send(1, buf2, 0, wide, mate).wait_recv()
        cnt_ref[...] = jnp.sum(buf2[...], axis=0)[:3]

    @pl.when(core == 1)
    def _():
        send(0, buf1, 0, 2 * near - 1, mate).wait_recv()
        part = jnp.sum(buf1[...], axis=0, keepdims=True)
        sbuf[1:2, :] = part
        buf2[wide - 1:wide, :] = part
        for k in plane:
            send(1, buf2, k - 1, 1, spread[k] + 1).start()
        for c in first:
            send(1, buf2, plane_no * length + spot, 1, c).start()
        send(0, buf1, 0, near - 1, mate).wait_send()
        send(1, buf2, 0, wide - 1, mate).wait_recv()
        whole = jnp.sum(buf2[...], axis=0, keepdims=True)
        cnt_ref[...] = whole[0, :3]

        @pl.when(plane_no > 0)
        def _():
            sbuf[2:3, :] = whole
            send(2, buf3, 0, 1, mate).start()
            send(2, buf3, 0, 1, mate).wait_send()

        send(1, buf2, 0, wide - 1, mate).wait_send()
        send(1, buf2, 0, len(first), mate).wait_send()


def write_kernel(sup, cnt, out, counts, sem):
    copies = [
        pltpu.make_async_copy(sup.at[pl.ds(64 * i, 64)], out.at[pl.ds(64 * i, 64)], sem.at[i])
        for i in range(8)
    ] + [pltpu.make_async_copy(cnt, counts, sem.at[8])]
    for c in copies:
        c.start()
    for c in copies:
        c.wait()


def group_size(axes):
    size = 1
    for _, s in axes:
        size *= s
    return size


def on_device(adj_diag, adj_right, alive_diag, alive_right, truss_k):
    n = lax.axis_size("rows")
    vmem = pl.BlockSpec(memory_space=pltpu.VMEM)
    smem = pl.BlockSpec(memory_space=pltpu.SMEM)
    hbm = pl.BlockSpec(memory_space=pl.ANY)
    tiles = [
        pltpu.with_memory_space_constraint(x, pltpu.HBM)
        for x in (adj_diag, adj_right, alive_diag, alive_right)
    ]
    support, counts = pl.pallas_call(
        lambda *refs: peel_kernel(n, *refs),
        out_shape=(
            pltpu.VMEM((TILE, 2 * TILE), F32),
            pltpu.VMEM((3,), I32),
        ),
        in_specs=[pl.BlockSpec(memory_space=pltpu.HBM)] * 4 + [smem],
        out_specs=[vmem, vmem],
        scratch_shapes=[
            pltpu.VMEM((4, WORDS, TILE), I32),
            pltpu.VMEM((HALF, WORDS, TILE), I32),
            pltpu.VMEM((HALF, len(PIECES) // 2, 8, 128), I32),
            pltpu.VMEM((2, HALF, TILE, TILE), F8),
            pltpu.VMEM((2, HALF, TILE, TILE), F8),
            pltpu.VMEM((TILE, TILE), F32),
            pltpu.VMEM((TILE, TILE), F32),
            pltpu.VMEM((3, 128), I32),
            pltpu.VMEM((2 * group_size(GATHER), 128), I32),
            pltpu.VMEM((group_size(SPREAD), 128), I32),
            pltpu.VMEM((1, 128), I32),
            pltpu.SemaphoreType.DMA((4,)),
            pltpu.SemaphoreType.DMA((6,)),
            pltpu.SemaphoreType.DMA((6,)),
            pltpu.SemaphoreType.DMA((3,)),
            pltpu.SemaphoreType.DMA((3,)),
        ],
        compiler_params=pltpu.CompilerParams(
            collective_id=0, has_side_effects=True, vmem_limit_bytes=40 * 2**20
        ),
        name="peel",
    )(*tiles, truss_k)
    return pl.pallas_call(
        write_kernel,
        out_shape=(
            jax.ShapeDtypeStruct((TILE, 2 * TILE), F32),
            jax.ShapeDtypeStruct((3,), I32),
        ),
        in_specs=[vmem, vmem],
        out_specs=[hbm, hbm],
        scratch_shapes=[pltpu.SemaphoreType.DMA((9,))],
        compiler_params=pltpu.CompilerParams(vmem_limit_bytes=4 * 2**20),
        name="write",
    )(support, counts)


def solution(mesh):
    rows = P("rows", None)
    return jax.shard_map(
        on_device, mesh=mesh, in_specs=(rows, rows, rows, rows, P(None)),
        out_specs=(rows, P(None)), check_vma=False,
    )
```
